32 devices in a mesh: groups: 2 (over y), ep: 4 (over z), sub: 4 (over x, core).
Axes of the slice: x: 2, y: 2, z: 4, core: 2. Of those that a mesh axis runs over, the one named last changes fastest.
Arguments:
- tokens: bfloat16 [512, 7168], P(('groups', 'ep'), 'sub'), parts along dimension 0, may hold values from -6 to 6
- expert_ids: int32 [512, 2], P(('groups', 'ep')), parts along dimension 0, may hold values from 0 to 3, all different within a row; in each aligned block of 64 rows (0 to 63, 64 to 127, ...) at most 48 rows name the same one
- route_weights: float32 [512, 2], P(('groups', 'ep')), parts along dimension 0, may hold values from 0.05 to 0.6
- gate_weight: bfloat16 [4, 7168, 1024], P('ep', 'sub'), may hold values from -0.0625 to 0.0625
- up_weight: bfloat16 [4, 7168, 1024], P('ep', 'sub'), may hold values from -0.0625 to 0.0625
- down_weight: bfloat16 [4, 1024, 7168], P('ep', None, 'sub'), may hold values from -0.1875 to 0.1875
- shared_gate: bfloat16 [1024, 7168], P('ep', 'sub'), may hold values from -0.0625 to 0.0625
- shared_up: bfloat16 [1024, 7168], P('ep', 'sub'), may hold values from -0.0625 to 0.0625
- shared_down: bfloat16 [1024, 7168], P('ep', 'sub'), may hold values from -0.1875 to 0.1875
Outputs:
- layer_out: bfloat16 [512, 7168], P(('groups', 'ep'), 'sub'), parts along dimension 0
The draws below stay inside these ranges and needn't reach their ends.
There are 2 independent parts, one for each index of `groups`. The reference program is written for one: setup_inputs(seed, part) draws one part's arguments, and reference() takes and returns one part's arrays. A program takes and returns all parts, laid end to end along the dimension named above; an argument that names none is the same for every part. Nothing has to cross between parts.
Inputs may be any that keep to these rules, and one draw needn't show every extreme that they name: `expert_ids`: each row names 2 different experts. Among the 64 rows of one ep index no expert is named more than 48 times, and in some of these aligned blocks an expert is named exactly 48 times.
All inputs are finite; a program needn't handle non-finite values.
Results may differ from the reference program's by a relative error of at most 0.0054.
Values may be sent and summed in bfloat16 or wider, within the bound.
No kernel may reach another device: no remote copies, remote signals or barrier semaphores. Data moves between devices by JAX's collectives and lax.ppermute only.
A program may use at most 128 MiB of HBM per device.

```python
import math
import jax
import jax.numpy as jnp
import numpy as np
from jax import lax

D = 7168
HIDDEN_SIZE = 1024
SH = 1024
TOK_EP = 64
EXPERTS = 4
TOPK = 2
CAP = 48
TOKENS = 256
N_EP = 4


def level_of(stream_key, shape, pieces, least, largest):
    def one(dim, shards_of):
        steps = jax.random.uniform(jax.random.fold_in(jax.random.fold_in(stream_key, 6), dim), (shards_of,), jnp.float32, least / len(pieces), largest / len(pieces))
        return jnp.repeat(jnp.exp(steps), shape[dim] // shards_of).reshape((-1,) + (1,) * (len(shape) - dim - 1))

    gain = one(*pieces[0])
    for cut in pieces[1:]:
        gain = gain * one(*cut)
    return gain


def deal_out(stream_key, own, number, rows, count, top, limit, lean):
    order = jax.random.permutation(stream_key, count)
    heavy_load, ordinary = portions_of(count, rows * top, limit, lean, True), portions_of(count, rows * top, limit, lean, False)
    places = jnp.arange(count)

    def named(lengths, offset_by):
        used = int((lengths > 0).sum())
        fixed = max(1, used // 4)
        moved = fixed + (places - fixed + offset_by * (used - fixed)) % max(1, count - fixed)
        return jnp.zeros((count,), jnp.int32).at[order[jnp.where(places < fixed, places, moved)]].set(jnp.asarray(lengths, jnp.int32))

    lengths = jnp.where(number % 4 == 0, named(heavy_load, number // 4), named(ordinary, number - number // 4 - 1))
    mixed = jax.random.permutation(jax.random.fold_in(own, 3), count)
    giver, sink = mixed[0:count // 2 * 2:2], mixed[1:count // 2 * 2:2]
    slack = jnp.minimum(lengths[giver] - 1, limit - lengths[sink]) // 2
    slack = jnp.where((giver == order[0]) | (sink == order[0]) | (lengths[sink] == 0), 0, jnp.maximum(slack, 0))
    moved = jax.random.randint(jax.random.fold_in(own, 4), (count // 2,), 0, 1 << 20) % (slack + 1)
    lengths = lengths.at[giver].add(-moved).at[sink].add(moved)
    labels = jnp.searchsorted(jnp.cumsum(lengths), jnp.arange(rows * top), side="right").astype(jnp.int32)
    grid = labels.reshape(top, rows).T
    grid = grid[jax.random.permutation(jax.random.fold_in(own, 1), rows)]
    offset_by = jax.random.randint(jax.random.fold_in(own, 2), (rows, 1), 0, top)
    return jnp.take_along_axis(grid, (jnp.arange(top)[None, :] + offset_by) % top, axis=1)


def portions_of(number_of, total, bound, lean, full):
    loads = [(1 << 20) // math.isqrt(rank ** lean) + 1 for rank in range(1, number_of + 1)]
    largest = bound if full else min(bound, max(-(-total // number_of), total * loads[0] // sum(loads)))
    least = 1 if total - largest >= number_of - 1 else 0
    counts, spare = [largest] + [least] * (number_of - 1), total - largest - least * (number_of - 1)
    while spare > 0:
        movable = [i for i in range(1, number_of) if counts[i] < largest] or [i for i in range(1, number_of) if counts[i] < bound]
        mass, left = sum([loads[i] for i in movable]), spare
        for i in movable:
            extra = min(bound - counts[i], max(1, left * loads[i] // mass), spare)
            counts[i] = counts[i] + extra
            spare = spare - extra
    return np.array(counts)


def centred(stream_key, extent, width, reach, split=(), kind=jnp.bfloat16):
    gain = level_of(stream_key, extent, split, -0.22, 0.18) if split else 1.0
    values = jax.random.normal(stream_key, extent, jnp.float32) * width * gain
    return jnp.minimum(jnp.maximum(values, -reach), reach).astype(kind)


def setup_inputs(seed: int = 0, part: int = 0) -> dict:
    key_of = jax.random.split(jax.random.key(seed), 10)
    part_keys = jax.random.split(jax.random.fold_in(key_of[9], part), 10)
    tokens = centred(part_keys[0], (TOKENS, D), 1.0, 6.0, ((0, 4), (1, 4)))
    expert_ids_keys = jax.random.split(jax.random.fold_in(part_keys[1], 1), TOKENS // TOK_EP)
    expert_ids_turns = jax.random.permutation(jax.random.fold_in(part_keys[1], 3), TOKENS // TOK_EP)
    expert_ids = jax.vmap(lambda own, number: deal_out(jax.random.fold_in(part_keys[1], 2), own, number, TOK_EP, EXPERTS, TOPK, CAP, 2))(expert_ids_keys, expert_ids_turns).reshape((TOKENS, TOPK))
    route_weights = jnp.clip(jnp.exp(math.log(0.6) - 2.4849067 * jax.random.uniform(part_keys[2], (TOKENS, TOPK), jnp.float32) ** level_of(part_keys[2], (TOKENS, TOPK), ((0, 4),), -0.2, 0.2)), 0.05, 0.6)
    gate_weight = centred(key_of[3], (EXPERTS, D, HIDDEN_SIZE), D ** -0.5, 0.0625, ((0, 4), (1, 4)))
    up_weight = centred(key_of[4], (EXPERTS, D, HIDDEN_SIZE), D ** -0.5, 0.0625, ((0, 4), (1, 4)))
    down_weight = centred(key_of[5], (EXPERTS, HIDDEN_SIZE, D), HIDDEN_SIZE ** -0.5, 0.1875, ((0, 4), (2, 4)))
    shared_gate = centred(key_of[6], (SH, D), D ** -0.5, 0.0625, ((0, 4), (1, 4)))
    shared_up = centred(key_of[7], (SH, D), D ** -0.5, 0.0625, ((0, 4), (1, 4)))
    shared_down = centred(key_of[8], (SH, D), SH ** -0.5, 0.1875, ((0, 4), (1, 4)))
    return {"tokens": tokens, "expert_ids": expert_ids, "route_weights": route_weights, "gate_weight": gate_weight, "up_weight": up_weight, "down_weight": down_weight, "shared_gate": shared_gate, "shared_up": shared_up, "shared_down": shared_down}


def reference(tokens, expert_ids, route_weights, gate_weight, up_weight, down_weight, shared_gate, shared_up, shared_down):
    contract = (((1,), (1,)), ((), ()))
    shared_pre = lax.dot_general(tokens, shared_gate, contract, preferred_element_type=jnp.float32)
    shared_lin = lax.dot_general(tokens, shared_up, contract, preferred_element_type=jnp.float32)
    shared_hidden = (jax.nn.silu(shared_pre) * shared_lin).astype(jnp.bfloat16)
    shared_out = jnp.dot(shared_hidden, shared_down, preferred_element_type=jnp.float32)
    most_rows = N_EP * CAP

    def expert_step(totals, inputs):
        gate_mat, up_mat, down_mat, expert = inputs
        chosen = expert_ids == expert
        weight_col = jnp.sum(jnp.where(chosen, route_weights, jnp.float32(0.0)), axis=1)
        absent = 1 - jnp.any(chosen, axis=1).astype(jnp.int32)
        row_order = jnp.argsort(absent, stable=True)[:most_rows].astype(jnp.int32)
        picked = tokens[row_order]
        expert_pre = jnp.dot(picked, gate_mat, preferred_element_type=jnp.float32)
        expert_lin = jnp.dot(picked, up_mat, preferred_element_type=jnp.float32)
        expert_hidden = (jax.nn.silu(expert_pre) * expert_lin).astype(jnp.bfloat16)
        expert_out = jnp.dot(expert_hidden, down_mat, preferred_element_type=jnp.float32).astype(jnp.bfloat16)
        totals = totals.at[row_order].add(weight_col[row_order][:, None] * expert_out.astype(jnp.float32))
        return totals, None

    expert_index = jnp.arange(EXPERTS, dtype=jnp.int32)
    routed, unused = lax.scan(expert_step, jnp.zeros((TOKENS, D), jnp.float32), (gate_weight, up_weight, down_weight, expert_index))
    return (shared_out + routed).astype(jnp.bfloat16)
```

```python
import jax
import jax.numpy as jnp
from jax import lax
from jax.sharding import PartitionSpec as P

WIRE = jnp.bfloat16
TOTAL = jnp.float32


def turn(value, axis, by):
    size = lax.axis_size(axis)
    return lax.ppermute(value, axis, [(i, (i + by) % size) for i in range(size)])


def swap(value, axis, bit):
    size = lax.axis_size(axis)
    return lax.ppermute(value, axis, [(i, i ^ bit) for i in range(size)])


def summed_rows(part):
    size, me = lax.axis_size("sub"), lax.axis_index("sub")
    bit = 1
    while bit * 2 < size:
        half = part.shape[0] // 2
        upper = (me & bit) != 0
        low, high = part[:half], part[half:]
        sent = jnp.where(upper, low, high).astype(WIRE)
        part = jnp.where(upper, high, low) + swap(sent, "sub", bit).astype(TOTAL)
        bit *= 2
    if bit < size:
        part = part + swap(part.astype(WIRE), "sub", bit).astype(TOTAL)
    return part


def gathered_rows(share):
    size, me = lax.axis_size("sub"), lax.axis_index("sub")
    bits = []
    b = 1
    while b * 2 < size:
        bits.append(b)
        b *= 2
    for b in reversed(bits):
        other = swap(share, "sub", b)
        upper = (me & b) != 0
        share = jnp.where(
            upper, jnp.concatenate([other, share]), jnp.concatenate([share, other])
        )
    return share


def per_device(
    tokens,
    expert_ids,
    route_weights,
    gate_weight,
    up_weight,
    down_weight,
    shared_gate,
    shared_up,
    shared_down,
):
    contract = (((1,), (1,)), ((), ()))
    experts = lax.axis_size("ep")
    me = lax.axis_index("ep")
    count = tokens.shape[0]
    hidden, narrow = gate_weight.shape[2], shared_gate.shape[0]
    blocks = [tokens] + [turn(tokens, "ep", k) for k in range(1, experts)]
    named = expert_ids[:, :, None] == jnp.arange(experts, dtype=jnp.int32)
    dense = jnp.sum(jnp.where(named, route_weights[:, :, None], 0.0), axis=1)
    scales = lax.all_gather(dense.T, "ep", axis=1, tiled=False)[me]
    chunks = [[0]] + [
        sorted({k, experts - k}) for k in range(1, experts // 2 + 1)
    ]
    answers = []
    for chunk in chunks:
        rows = jnp.concatenate([blocks[k] for k in chunk])
        parts = [
            jnp.dot(rows, gate_weight[0], preferred_element_type=TOTAL),
            jnp.dot(rows, up_weight[0], preferred_element_type=TOTAL),
            lax.dot_general(rows, shared_gate, contract, preferred_element_type=TOTAL),
            lax.dot_general(rows, shared_up, contract, preferred_element_type=TOTAL),
        ]
        full = summed_rows(jnp.concatenate(parts, axis=1))
        pre, lin = full[:, :hidden], full[:, hidden : 2 * hidden]
        pre_s, lin_s = full[:, 2 * hidden : -narrow], full[:, -narrow:]
        act = jnp.concatenate(
            [jax.nn.silu(pre) * lin, jax.nn.silu(pre_s) * lin_s], axis=1
        ).astype(jnp.bfloat16)
        act = gathered_rows(act)
        scale = jnp.concatenate([scales[(me - k) % experts] for k in chunk])
        out = jnp.dot(act[:, hidden:], shared_down, preferred_element_type=TOTAL)
        out = out + scale[:, None] * jnp.dot(
            act[:, :hidden], down_weight[0], preferred_element_type=TOTAL
        )
        for place, k in enumerate(chunk):
            piece = out[place * count : (place + 1) * count]
            answers.append(piece if k == 0 else turn(piece.astype(WIRE), "ep", -k))
    total = answers[0]
    for answer in answers[1:]:
        total = total + answer.astype(TOTAL)
    return total.astype(jnp.bfloat16)


def solution(mesh):
    in_specs = (
        P(("groups", "ep"), "sub"),
        P(("groups", "ep"), None),
        P(("groups", "ep"), None),
        P("ep", "sub", None),
        P("ep", "sub", None),
        P("ep", None, "sub"),
        P("ep", "sub"),
        P("ep", "sub"),
        P("ep", "sub"),
    )
    out_specs = P(("groups", "ep"), "sub")
    return jax.shard_map(
        per_device, mesh=mesh, in_specs=in_specs, out_specs=out_specs, check_vma=False
    )
```

```python
import jax
import jax.numpy as jnp
from jax import lax
from jax.experimental import pallas as pl
from jax.experimental.pallas import tpu as pltpu
from jax.sharding import PartitionSpec as P

WIRE = jnp.bfloat16
TOTAL = jnp.float32
COLUMNS = 256
NN = (((1,), (0,)), ((), ()))
NT = (((1,), (1,)), ((), ()))
VMEM = pl.BlockSpec(memory_space=pltpu.VMEM)
MIB = 1 << 20


def swap(value, axis, mask):
    size = lax.axis_size(axis)
    return lax.ppermute(value, axis, [(i, i ^ mask) for i in range(size)])


def tiles(width):
    step = COLUMNS if width % COLUMNS == 0 else width
    return [slice(at, at + step) for at in range(0, width, step)]


def nbytes(arrays):
    return sum(a.size * a.dtype.itemsize for a in arrays)


def call(kernel, out_shape, operands, flops, spare=4 * MIB, held=()):
    moved = nbytes(operands) + nbytes(out_shape)
    held = [pltpu.with_memory_space_constraint(w, pltpu.VMEM) for w in held]
    return pl.pallas_call(
        kernel,
        out_shape=out_shape,
        in_specs=[VMEM] * (len(operands) + len(held)),
        out_specs=[VMEM] * len(out_shape),
        compiler_params=pltpu.CompilerParams(vmem_limit_bytes=moved + spare),
        cost_estimate=pl.CostEstimate(
            flops=flops, bytes_accessed=moved, transcendentals=0
        ),
    )(*operands, *held)


def keeps_high():
    return (lax.axis_index("sub") & 1) != 0


def project_rows(rows_refs, weights, sent_ref, kept_ref, ready):
    half = sent_ref.shape[0]
    rows = jnp.concatenate([ref[...] for ref in rows_refs])
    low, high = rows[:half], rows[half:]
    rows = jnp.concatenate(
        [jnp.where(keeps_high(), low, high), jnp.where(keeps_high(), high, low)]
    )
    at = 0
    for k, weight_ref in enumerate(weights):
        ready(k)
        straight = len(weight_ref.shape) == 3
        for cut in tiles(weight_ref.shape[2 if straight else 0]):
            weight = weight_ref[0, :, cut] if straight else weight_ref[cut, :]
            part = lax.dot_general(
                rows, weight, NN if straight else NT, preferred_element_type=TOTAL
            )
            width = cut.stop - cut.start
            sent_ref[:, at : at + width] = part[:half]
            kept_ref[:, at : at + width] = part[half:]
            at += width


def halves(rows, weights):
    count, depth = sum(r.shape[0] for r in rows), rows[0].shape[1]
    width = 2 * weights[0].shape[2] + 2 * weights[2].shape[0]
    half = jax.ShapeDtypeStruct((count // 2, width), TOTAL)
    return [half, half], 2 * count * depth * width


def open_chunk(rows, weights):
    shapes, flops = halves(rows, weights)
    spread, many = len(rows), len(weights)

    def kernel(*refs):
        sources = refs[spread : spread + many]
        sent_ref, kept_ref, *held = refs[spread + many : -1]
        copies = [
            pltpu.make_async_copy(source, target, refs[-1].at[k])
            for k, (source, target) in enumerate(zip(sources, held, strict=True))
        ]
        for copy in copies:
            copy.start()
        project_rows(
            refs[:spread], held[:4], sent_ref, kept_ref, lambda k: copies[k].wait()
        )
        for copy in copies[4:]:
            copy.wait()

    moved = nbytes(weights)
    sent, kept, *held = pl.pallas_call(
        kernel,
        out_shape=shapes + [pltpu.VMEM(w.shape, w.dtype) for w in weights],
        in_specs=[VMEM] * spread + [pl.BlockSpec(memory_space=pl.ANY)] * many,
        out_specs=[VMEM] * (2 + many),
        scratch_shapes=[pltpu.SemaphoreType.DMA((many,))],
        compiler_params=pltpu.CompilerParams(
            vmem_limit_bytes=moved + nbytes(rows) + nbytes(shapes) + 8 * MIB
        ),
        cost_estimate=pl.CostEstimate(
            flops=flops, bytes_accessed=moved, transcendentals=0
        ),
    )(*rows, *[pltpu.with_memory_space_constraint(w, pltpu.HBM) for w in weights])
    return sent, kept, held


def project(rows, weights):
    def kernel(*refs):
        count = len(rows)
        project_rows(refs[:count], refs[count : count + 4], *refs[-2:], lambda k: None)

    shapes, flops = halves(rows, weights)
    return call(kernel, shapes, rows, flops, held=weights[:4])


def total_of(refs):
    total = refs[0][...]
    for ref in refs[1:]:
        total = total + ref[...].astype(TOTAL)
    return total


def added(parts):
    def kernel(*refs):
        refs[-1][...] = total_of(refs[:-1]).astype(WIRE)

    shape = jax.ShapeDtypeStruct(parts[0].shape, WIRE)
    return call(kernel, [shape], parts, parts[0].size * 4096)[0]


def activated(parts, hidden):
    rows, width = parts[0].shape

    def kernel(*refs):
        full, out_ref = total_of(refs[:-1]), refs[-1]
        edge = (width - 2 * hidden) // 2
        for at, size, to in ((0, hidden, 0), (2 * hidden, edge, hidden)):
            pre, lin = full[:, at : at + size], full[:, at + size : at + 2 * size]
            value = pre / (1.0 + jnp.exp(-pre)) * lin
            out_ref[:, to : to + size] = value.astype(out_ref.dtype)

    shape = jax.ShapeDtypeStruct((rows, width // 2), jnp.bfloat16)
    return call(kernel, [shape], parts, parts[0].size * 4096)[0]


def finish(mine, other, scales, places, weights, dtypes):
    down, _ = weights[4:]
    rows, width = 2 * mine.shape[0], down.shape[2]
    count = rows // len(places)

    def kernel(mine_ref, other_ref, scales_ref, down_ref, sdown_ref, *out_refs):
        hidden = down_ref.shape[1]
        mine, other = mine_ref[...], other_ref[...]
        act = jnp.concatenate(
            [
                jnp.where(keeps_high(), other, mine),
                jnp.where(keeps_high(), mine, other),
            ]
        )
        square = (count, count)
        here = lax.broadcasted_iota(jnp.int32, square, 0)
        here = here == lax.broadcasted_iota(jnp.int32, square, 1)
        expert = lax.axis_index("ep")
        scale = []
        for place in places:
            line = scales_ref[place, pl.ds(expert, 1), :]
            spread = jnp.where(here, jnp.broadcast_to(line, square), 0.0)
            scale.append(jnp.sum(spread, axis=1, keepdims=True))
        scale = jnp.concatenate(scale)
        for cut in tiles(width):
            routed = jnp.dot(
                act[:, :hidden], down_ref[0, :, cut], preferred_element_type=TOTAL
            )
            shared = jnp.dot(
                act[:, hidden:], sdown_ref[:, cut], preferred_element_type=TOTAL
            )
            out = shared + scale * routed
            for at, out_ref in enumerate(out_refs):
                piece = out[at * count : (at + 1) * count]
                out_ref[:, cut] = piece.astype(out_ref.dtype)

    return call(
        kernel,
        [jax.ShapeDtypeStruct((count, width), dtype) for dtype in dtypes],
        [mine, other, scales],
        2 * rows * mine.shape[1] * width,
        held=weights[4:],
    )


def group(masks):
    if len(masks) < 4:
        return [[m] for m in masks]
    step = len(masks) // 4
    own, across, near, far = [masks[at : at + step] for at in range(0, 4 * step, step)]
    return [own, across, far, near]


def per_device(
    tokens,
    expert_ids,
    route_weights,
    gate_weight,
    up_weight,
    down_weight,
    shared_gate,
    shared_up,
    shared_down,
):
    experts, sub = lax.axis_size("ep"), lax.axis_size("sub")
    hidden = gate_weight.shape[2]
    bits = [1 << b for b in reversed(range(experts.bit_length() - 1))]
    weights = [gate_weight, up_weight, shared_gate, shared_up, down_weight, shared_down]

    named = expert_ids.T[:, None, :] == jnp.arange(experts, dtype=jnp.int32)[:, None]
    dense = jnp.sum(jnp.where(named, route_weights.T[:, None, :], 0.0), axis=0)
    blocks, masks, scales = {0: tokens}, [0], dense[None]
    for bit in bits:
        for m in list(masks):
            blocks[m | bit] = swap(blocks[m], "ep", bit)
        masks = masks + [m | bit for m in masks]
        scales = jnp.concatenate([scales, swap(scales, "ep", bit)])

    answers = {}
    for k, chunk in enumerate(group(masks)):
        rows = [blocks[m] for m in chunk]
        if k == 0:
            sent, kept, weights = open_chunk(rows, weights)
        else:
            sent, kept = project(rows, weights)
        parts = [kept, swap(sent, "sub", 1)]
        bit = 2
        while bit < sub:
            wire = added(parts)
            parts.append(swap(wire, "sub", bit))
            bit *= 2
        mine = activated(parts, hidden)
        other = swap(mine, "sub", 1)
        places = [masks.index(m) for m in chunk]
        dtypes = [WIRE if m else TOTAL for m in chunk]
        out = finish(mine, other, scales, places, weights, dtypes)
        for m, piece in zip(chunk, out, strict=True):
            answers[m] = swap(piece, "ep", m) if m else piece
    total = answers[0]
    for m in masks[1:]:
        total = total + answers[m].astype(TOTAL)
    return total.astype(jnp.bfloat16)


def solution(mesh):
    in_specs = (
        P(("groups", "ep"), "sub"),
        P(("groups", "ep"), None),
        P(("groups", "ep"), None),
        P("ep", "sub", None),
        P("ep", "sub", None),
        P("ep", None, "sub"),
        P("ep", "sub"),
        P("ep", "sub"),
        P("ep", "sub"),
    )
    out_specs = P(("groups", "ep"), "sub")

    return jax.shard_map(
        per_device, mesh=mesh, in_specs=in_specs, out_specs=out_specs, check_vma=False
    )
```

```python
import jax
import jax.numpy as jnp
from jax import lax
from jax.experimental import pallas as pl
from jax.experimental.pallas import tpu as pltpu
from jax.sharding import PartitionSpec as P

WIRE = jnp.bfloat16
TOTAL = jnp.float32
COLUMNS = 256
NN = (((1,), (0,)), ((), ()))
NT = (((1,), (1,)), ((), ()))
VMEM = pl.BlockSpec(memory_space=pltpu.VMEM)
MIB = 1 << 20


def swap(value, axis, mask):
    size = lax.axis_size(axis)
    return lax.ppermute(value, axis, [(i, i ^ mask) for i in range(size)])


def tiles(width):
    step = COLUMNS if width % COLUMNS == 0 else width
    return [slice(at, at + step) for at in range(0, width, step)]


def nbytes(arrays):
    return sum(a.size * a.dtype.itemsize for a in arrays)


def call(kernel, out_shape, operands, flops, spare=4 * MIB, held=()):
    moved = nbytes(operands) + nbytes(out_shape)
    held = [pltpu.with_memory_space_constraint(w, pltpu.VMEM) for w in held]
    return pl.pallas_call(
        kernel,
        out_shape=out_shape,
        in_specs=[VMEM] * (len(operands) + len(held)),
        out_specs=[VMEM] * len(out_shape),
        compiler_params=pltpu.CompilerParams(vmem_limit_bytes=moved + spare),
        cost_estimate=pl.CostEstimate(
            flops=flops, bytes_accessed=moved, transcendentals=0
        ),
    )(*operands, *held)


def keeps_high():
    return (lax.axis_index("sub") & 1) != 0


def project_rows(blocks, weights, sent_refs, kept_ref, ready):
    half = blocks[0].shape[0] // 2
    low = jnp.concatenate([block[:half] for block in blocks])
    high = jnp.concatenate([block[half:] for block in blocks])
    rows = jnp.concatenate(
        [jnp.where(keeps_high(), low, high), jnp.where(keeps_high(), high, low)]
    )
    half, at = kept_ref.shape[0], 0
    for k, weight_ref in enumerate(weights):
        ready(k)
        straight = len(weight_ref.shape) == 3
        for cut in tiles(weight_ref.shape[2 if straight else 0]):
            weight = weight_ref[0, :, cut] if straight else weight_ref[cut, :]
            part = lax.dot_general(
                rows, weight, NN if straight else NT, preferred_element_type=TOTAL
            )
            width = cut.stop - cut.start
            row = 0
            for sent_ref in sent_refs:
                end = row + sent_ref.shape[0]
                sent_ref[:, at : at + width] = part[row:end]
                row = end
            kept_ref[:, at : at + width] = part[half:]
            at += width


def halves(lanes, weights):
    (count, depth), width = (
        lanes[0][0].shape,
        2 * (weights[0].shape[2] + weights[2].shape[0]),
    )
    sizes = [len(lane) * count // 2 for lane in lanes]
    shapes = [
        jax.ShapeDtypeStruct((size, width), TOTAL) for size in (*sizes, sum(sizes))
    ]
    return shapes, 4 * sum(sizes) * depth * width


def open_chunk(lanes, weights):
    shapes, flops = halves(lanes, weights)
    rows = [block for lane in lanes for block in lane]
    spread, many = len(rows), len(weights)

    def kernel(*refs):
        sources, made = refs[: spread + many], refs[spread + many : -2]
        (*sent_refs, kept_ref), held = made[: len(shapes)], list(made[len(shapes) :])
        rows_ref, sems = refs[-2:]
        targets = [rows_ref.at[k] for k in range(spread)] + held
        copies = [
            pltpu.make_async_copy(source, target, sems.at[k])
            for k, (source, target) in enumerate(zip(sources, targets, strict=True))
        ]
        for copy in copies:
            copy.start()
        for copy in copies[:spread]:
            copy.wait()
        blocks = [rows_ref[k] for k in range(spread)]
        project_rows(
            blocks, held[:4], sent_refs, kept_ref, lambda k: copies[spread + k].wait()
        )
        for copy in copies[spread + 4 :]:
            copy.wait()

    moved = nbytes(weights) + nbytes(rows)
    sources = [pltpu.with_memory_space_constraint(a, pltpu.HBM) for a in rows + weights]
    made = pl.pallas_call(
        kernel,
        out_shape=shapes + [pltpu.VMEM(w.shape, w.dtype) for w in weights],
        in_specs=[pl.BlockSpec(memory_space=pl.ANY)] * (spread + many),
        out_specs=[VMEM] * (len(shapes) + many),
        scratch_shapes=[
            pltpu.VMEM((spread, *rows[0].shape), rows[0].dtype),
            pltpu.SemaphoreType.DMA((spread + many,)),
        ],
        compiler_params=pltpu.CompilerParams(
            vmem_limit_bytes=moved + nbytes(shapes) + 8 * MIB
        ),
        cost_estimate=pl.CostEstimate(
            flops=flops, bytes_accessed=moved, transcendentals=0
        ),
    )(*sources)
    return made[: len(shapes)], list(made[len(shapes) :])


def project(lanes, weights):
    shapes, flops = halves(lanes, weights)
    rows = [block for lane in lanes for block in lane]
    count = len(rows)

    def kernel(*refs):
        blocks = [ref[...] for ref in refs[:count]]
        *sent_refs, kept_ref = refs[count + 4 :]
        project_rows(
            blocks, refs[count : count + 4], sent_refs, kept_ref, lambda k: None
        )

    return call(kernel, shapes, rows, flops, held=weights[:4])


def total_of(refs, lane):
    total = refs[0][lane, :]
    for ref in refs[1:]:
        total = total + ref[...].astype(TOTAL)
    return total


def added(parts, lane):
    def kernel(*refs):
        refs[-1][...] = total_of(refs[:-1], lane).astype(WIRE)

    shape = jax.ShapeDtypeStruct((lane.stop - lane.start, parts[0].shape[1]), WIRE)
    return call(kernel, [shape], parts, shape.size * 4096)[0]


def activated(parts, lane, hidden):
    width = parts[0].shape[1]

    def kernel(*refs):
        full, out_ref = total_of(refs[:-1], lane), refs[-1]
        edge = (width - 2 * hidden) // 2
        for at, size, to in ((0, hidden, 0), (2 * hidden, edge, hidden)):
            pre, lin = full[:, at : at + size], full[:, at + size : at + 2 * size]
            value = pre / (1.0 + jnp.exp(-pre)) * lin
            out_ref[:, to : to + size] = value.astype(out_ref.dtype)

    shape = jax.ShapeDtypeStruct((lane.stop - lane.start, width // 2), jnp.bfloat16)
    return call(kernel, [shape], parts, shape.size * 4096)[0]


def merged(piece, carried):
    def kernel(piece_ref, carried_ref, out_ref):
        out_ref[...] = (piece_ref[...] + carried_ref[...].astype(TOTAL)).astype(WIRE)

    shape = jax.ShapeDtypeStruct(piece.shape, WIRE)
    return call(kernel, [shape], [piece, carried], piece.size * 4096)[0]


def finish(mine, other, scales, places, weights, dtypes):
    down, _ = weights[4:]
    rows, width = 2 * mine.shape[0], down.shape[2]
    count = rows // len(places)

    def kernel(mine_ref, other_ref, scales_ref, down_ref, sdown_ref, *out_refs):
        hidden = down_ref.shape[1]
        mine, other = mine_ref[...], other_ref[...]
        low = jnp.where(keeps_high(), other, mine)
        high = jnp.where(keeps_high(), mine, other)
        cuts = [slice(at, at + count // 2) for at in range(0, rows // 2, count // 2)]
        act = jnp.concatenate([side[cut] for cut in cuts for side in (low, high)])
        square = (count, count)
        here = lax.broadcasted_iota(jnp.int32, square, 0)
        here = here == lax.broadcasted_iota(jnp.int32, square, 1)
        expert = lax.axis_index("ep")
        scale = []
        for place in places:
            line = scales_ref[place, pl.ds(expert, 1), :]
            spread = jnp.where(here, jnp.broadcast_to(line, square), 0.0)
            scale.append(jnp.sum(spread, axis=1, keepdims=True))
        scale = jnp.concatenate(scale)
        for cut in tiles(width):
            routed = jnp.dot(
                act[:, :hidden], down_ref[0, :, cut], preferred_element_type=TOTAL
            )
            shared = jnp.dot(
                act[:, hidden:], sdown_ref[:, cut], preferred_element_type=TOTAL
            )
            out = shared + scale * routed
            for at, out_ref in enumerate(out_refs):
                piece = out[at * count : (at + 1) * count]
                out_ref[:, cut] = piece.astype(out_ref.dtype)

    return call(
        kernel,
        [jax.ShapeDtypeStruct((count, width), dtype) for dtype in dtypes],
        [mine, other, scales],
        2 * rows * mine.shape[1] * width,
        held=weights[4:],
    )


def group(masks):
    if len(masks) < 4:
        return [[[m]] for m in masks]
    step = len(masks) // 4
    own, across, near, far = [masks[at : at + step] for at in range(0, 4 * step, step)]
    return [[own], [across, near], [far]]


def per_device(
    tokens,
    expert_ids,
    route_weights,
    gate_weight,
    up_weight,
    down_weight,
    shared_gate,
    shared_up,
    shared_down,
):
    experts, sub = lax.axis_size("ep"), lax.axis_size("sub")
    hidden = gate_weight.shape[2]
    bits = [1 << b for b in reversed(range(experts.bit_length() - 1))]
    weights = [gate_weight, up_weight, shared_gate, shared_up, down_weight, shared_down]

    named = expert_ids.T[:, None, :] == jnp.arange(experts, dtype=jnp.int32)[:, None]
    dense = jnp.sum(jnp.where(named, route_weights.T[:, None, :], 0.0), axis=0)
    blocks, masks, scales = {0: tokens}, [0], dense[None]
    for step, bit in enumerate(bits):
        for m in list(masks):
            blocks[m | bit] = swap(blocks[m], "ep", bit)
        masks = masks + [m | bit for m in masks]
        scales = jnp.concatenate([scales, swap(scales, "ep", bit)])

    answers, passed, number = {}, {}, 0
    step = experts // 4
    for k, lanes in enumerate(group(masks)):
        rows = [[blocks[m] for m in lane] for lane in lanes]
        if k == 0:
            made, weights = open_chunk(rows, weights)
        else:
            made = project(rows, weights)
        at = 0
        for chunk, sent in zip(lanes, made[:-1], strict=True):
            lane = slice(at, at + sent.shape[0])
            parts = [made[-1], swap(sent, "sub", 1)]
            at, bit = lane.stop, 2
            while bit < sub:
                wire = added(parts, lane)
                parts.append(swap(wire, "sub", bit))
                bit *= 2
            mine = activated(parts, lane, hidden)
            other = swap(mine, "sub", 1)
            places = [masks.index(m) for m in chunk]
            dtypes = [TOTAL if m == 0 or m in passed else WIRE for m in chunk]
            out = finish(mine, other, scales, places, weights, dtypes)
            for m, piece in zip(chunk, out, strict=True):
                if m in passed:
                    piece = merged(piece, passed[m])
                if step and number == 1:
                    passed[m | step] = swap(piece, "ep", step)
                else:
                    answers[m] = swap(piece, "ep", m) if m else piece
            number += 1
    total = answers[0]
    for m in sorted(answers)[1:]:
        total = total + answers[m].astype(TOTAL)
    return total.astype(jnp.bfloat16)


def solution(mesh):
    in_specs = (
        P(("groups", "ep"), "sub"),
        P(("groups", "ep"), None),
        P(("groups", "ep"), None),
        P("ep", "sub", None),
        P("ep", "sub", None),
        P("ep", None, "sub"),
        P("ep", "sub"),
        P("ep", "sub"),
        P("ep", "sub"),
    )
    out_specs = P(("groups", "ep"), "sub")

    return jax.shard_map(
        per_device, mesh=mesh, in_specs=in_specs, out_specs=out_specs, check_vma=False
    )
```

```python
import jax
import jax.numpy as jnp
from jax import lax
from jax.experimental import pallas as pl
from jax.experimental.pallas import tpu as pltpu
from jax.sharding import PartitionSpec as P

WIRE = jnp.bfloat16
TOTAL = jnp.float32
COLUMNS = 256
FULL = 128
NN = (((1,), (0,)), ((), ()))
NT = (((1,), (1,)), ((), ()))
VMEM = pl.BlockSpec(memory_space=pltpu.VMEM)
MIB = 1 << 20


def swap(value, axis, mask):
    size = lax.axis_size(axis)
    return lax.ppermute(value, axis, [(i, i ^ mask) for i in range(size)])


def tiles(width):
    step = COLUMNS if width % COLUMNS == 0 else width
    return [slice(at, at + step) for at in range(0, width, step)]


def nbytes(arrays):
    return sum(a.size * a.dtype.itemsize for a in arrays)


def call(kernel, out_shape, operands, flops, spare=4 * MIB, held=()):
    moved = nbytes(operands) + nbytes(out_shape)
    held = [pltpu.with_memory_space_constraint(w, pltpu.VMEM) for w in held]
    return pl.pallas_call(
        kernel,
        out_shape=out_shape,
        in_specs=[VMEM] * (len(operands) + len(held)),
        out_specs=[VMEM] * len(out_shape),
        compiler_params=pltpu.CompilerParams(vmem_limit_bytes=moved + spare),
        cost_estimate=pl.CostEstimate(
            flops=flops, bytes_accessed=moved, transcendentals=0
        ),
    )(*operands, *held)


def keeps_high():
    return (lax.axis_index("sub") & 1) != 0


def project_rows(blocks, weights, sent_refs, kept_ref, ready):
    half = blocks[0].shape[0] // 2
    low = jnp.concatenate([block[:half] for block in blocks])
    high = jnp.concatenate([block[half:] for block in blocks])
    rows = jnp.concatenate(
        [jnp.where(keeps_high(), low, high), jnp.where(keeps_high(), high, low)]
    )
    half, at = kept_ref.shape[0], 0
    if rows.shape[0] < FULL:
        rows = jnp.concatenate([rows] * (FULL // rows.shape[0]))
    for k, weight_ref in enumerate(weights):
        ready(k)
        straight = len(weight_ref.shape) == 3
        for cut in tiles(weight_ref.shape[2 if straight else 0]):
            weight = weight_ref[0, :, cut] if straight else weight_ref[cut, :]
            part = lax.dot_general(
                rows, weight, NN if straight else NT, preferred_element_type=TOTAL
            )
            width = cut.stop - cut.start
            row = 0
            for sent_ref in sent_refs:
                end = row + sent_ref.shape[0]
                sent_ref[:, at : at + width] = part[row:end]
                row = end
            kept_ref[:, at : at + width] = part[half : 2 * half]
            at += width


def halves(lanes, weights):
    (count, depth), width = (
        lanes[0][0].shape,
        2 * (weights[0].shape[2] + weights[2].shape[0]),
    )
    sizes = [len(lane) * count // 2 for lane in lanes]
    shapes = [
        jax.ShapeDtypeStruct((size, width), TOTAL) for size in (*sizes, sum(sizes))
    ]
    return shapes, 4 * sum(sizes) * depth * width


def open_chunk(lanes, weights):
    shapes, flops = halves(lanes, weights)
    rows = [block for lane in lanes for block in lane]
    spread, many = len(rows), len(weights)

    def kernel(*refs):
        sources, made = refs[: spread + many], refs[spread + many : -2]
        (*sent_refs, kept_ref), held = made[: len(shapes)], list(made[len(shapes) :])
        rows_ref, sems = refs[-2:]
        targets = [rows_ref.at[k] for k in range(spread)] + held
        copies = [
            pltpu.make_async_copy(source, target, sems.at[k])
            for k, (source, target) in enumerate(zip(sources, targets, strict=True))
        ]
        for copy in copies:
            copy.start()
        for copy in copies[:spread]:
            copy.wait()
        blocks = [rows_ref[k] for k in range(spread)]
        project_rows(
            blocks, held[:4], sent_refs, kept_ref, lambda k: copies[spread + k].wait()
        )
        for copy in copies[spread + 4 :]:
            copy.wait()

    moved = nbytes(weights) + nbytes(rows)
    sources = [pltpu.with_memory_space_constraint(a, pltpu.HBM) for a in rows + weights]
    made = pl.pallas_call(
        kernel,
        out_shape=shapes + [pltpu.VMEM(w.shape, w.dtype) for w in weights],
        in_specs=[pl.BlockSpec(memory_space=pl.ANY)] * (spread + many),
        out_specs=[VMEM] * (len(shapes) + many),
        scratch_shapes=[
            pltpu.VMEM((spread, *rows[0].shape), rows[0].dtype),
            pltpu.SemaphoreType.DMA((spread + many,)),
        ],
        compiler_params=pltpu.CompilerParams(
            vmem_limit_bytes=moved + nbytes(shapes) + 8 * MIB
        ),
        cost_estimate=pl.CostEstimate(
            flops=flops, bytes_accessed=moved, transcendentals=0
        ),
    )(*sources)
    return made[: len(shapes)], list(made[len(shapes) :])


def project(lanes, weights):
    shapes, flops = halves(lanes, weights)
    rows = [block for lane in lanes for block in lane]
    count = len(rows)

    def kernel(*refs):
        blocks = [ref[...] for ref in refs[:count]]
        *sent_refs, kept_ref = refs[count + 4 :]
        project_rows(
            blocks, refs[count : count + 4], sent_refs, kept_ref, lambda k: None
        )

    return call(kernel, shapes, rows, flops, held=weights[:4])


def total_of(refs, lane):
    total = refs[0][lane, :]
    for ref in refs[1:]:
        total = total + ref[...].astype(TOTAL)
    return total


def added(parts, lane):
    def kernel(*refs):
        refs[-1][...] = total_of(refs[:-1], lane).astype(WIRE)

    shape = jax.ShapeDtypeStruct((lane.stop - lane.start, parts[0].shape[1]), WIRE)
    return call(kernel, [shape], parts, shape.size * 4096)[0]


def activated(parts, lane, hidden):
    width = parts[0].shape[1]

    def kernel(*refs):
        full, out_ref = total_of(refs[:-1], lane), refs[-1]
        edge = (width - 2 * hidden) // 2
        for at, size, to in ((0, hidden, 0), (2 * hidden, edge, hidden)):
            pre, lin = full[:, at : at + size], full[:, at + size : at + 2 * size]
            value = pre / (1.0 + jnp.exp(-pre)) * lin
            out_ref[:, to : to + size] = value.astype(out_ref.dtype)

    shape = jax.ShapeDtypeStruct((lane.stop - lane.start, width // 2), jnp.bfloat16)
    return call(kernel, [shape], parts, shape.size * 4096)[0]


def merged(piece, carried):
    def kernel(piece_ref, carried_ref, out_ref):
        out_ref[...] = (piece_ref[...] + carried_ref[...].astype(TOTAL)).astype(WIRE)

    shape = jax.ShapeDtypeStruct(piece.shape, WIRE)
    return call(kernel, [shape], [piece, carried], piece.size * 4096)[0]


def finish(mine, other, scales, places, weights, dtypes):
    down, _ = weights[4:]
    rows, width = 2 * mine.shape[0], down.shape[2]
    count = rows // len(places)

    def kernel(mine_ref, other_ref, scales_ref, down_ref, sdown_ref, *out_refs):
        hidden = down_ref.shape[1]
        mine, other = mine_ref[...], other_ref[...]
        low = jnp.where(keeps_high(), other, mine)
        high = jnp.where(keeps_high(), mine, other)
        cuts = [slice(at, at + count // 2) for at in range(0, rows // 2, count // 2)]
        act = jnp.concatenate([side[cut] for cut in cuts for side in (low, high)])
        if rows < FULL:
            act = jnp.concatenate([act] * (FULL // rows))
        square = (count, count)
        here = lax.broadcasted_iota(jnp.int32, square, 0)
        here = here == lax.broadcasted_iota(jnp.int32, square, 1)
        expert = lax.axis_index("ep")
        scale = []
        for place in places:
            line = scales_ref[place, pl.ds(expert, 1), :]
            spread = jnp.where(here, jnp.broadcast_to(line, square), 0.0)
            scale.append(jnp.sum(spread, axis=1, keepdims=True))
        scale = jnp.concatenate(scale)
        for cut in tiles(width):
            routed = jnp.dot(
                act[:, :hidden], down_ref[0, :, cut], preferred_element_type=TOTAL
            )
            shared = jnp.dot(
                act[:, hidden:], sdown_ref[:, cut], preferred_element_type=TOTAL
            )
            out = shared[:rows] + scale * routed[:rows]
            for at, out_ref in enumerate(out_refs):
                piece = out[at * count : (at + 1) * count]
                out_ref[:, cut] = piece.astype(out_ref.dtype)

    return call(
        kernel,
        [jax.ShapeDtypeStruct((count, width), dtype) for dtype in dtypes],
        [mine, other, scales],
        2 * rows * mine.shape[1] * width,
        held=weights[4:],
    )


def group(masks):
    if len(masks) < 4:
        return [[[m]] for m in masks]
    near = len(masks) // 4

    def lane(high):
        return [m for m in masks if m & 3 * near == high]

    return [[lane(0)], [lane(2 * near), lane(near)], [lane(3 * near)]]


def per_device(
    tokens,
    expert_ids,
    route_weights,
    gate_weight,
    up_weight,
    down_weight,
    shared_gate,
    shared_up,
    shared_down,
):
    experts, sub = lax.axis_size("ep"), lax.axis_size("sub")
    hidden = gate_weight.shape[2]
    bits = [1 << b for b in reversed(range(experts.bit_length() - 1))]
    weights = [gate_weight, up_weight, shared_gate, shared_up, down_weight, shared_down]

    named = expert_ids.T[:, None, :] == jnp.arange(experts, dtype=jnp.int32)[:, None]
    dense = jnp.sum(jnp.where(named, route_weights.T[:, None, :], 0.0), axis=0)
    blocks, masks, scales = {0: tokens}, [0], dense[None]
    for step, bit in enumerate(bits):
        for m in list(masks):
            blocks[m | bit] = swap(blocks[m], "ep", bit)
        masks = masks + [m | bit for m in masks]
        scales = jnp.concatenate([scales, swap(scales, "ep", bit)])

    answers, passed, number = {}, {}, 0
    step = experts // 4
    for k, lanes in enumerate(group(masks)):
        rows = [[blocks[m] for m in lane] for lane in lanes]
        if k == 0:
            made, weights = open_chunk(rows, weights)
        else:
            made = project(rows, weights)
        at = 0
        for chunk, sent in zip(lanes, made[:-1], strict=True):
            lane = slice(at, at + sent.shape[0])
            parts = [made[-1], swap(sent, "sub", 1)]
            at, bit = lane.stop, 2
            while bit < sub:
                wire = added(parts, lane)
                parts.append(swap(wire, "sub", bit))
                bit *= 2
            mine = activated(parts, lane, hidden)
            other = swap(mine, "sub", 1)
            places = [masks.index(m) for m in chunk]
            dtypes = [TOTAL if m == 0 or m in passed else WIRE for m in chunk]
            out = finish(mine, other, scales, places, weights, dtypes)
            for m, piece in zip(chunk, out, strict=True):
                if m in passed:
                    piece = merged(piece, passed[m])
                if step and number == 1:
                    passed[m | step] = swap(piece, "ep", step)
                else:
                    answers[m] = swap(piece, "ep", m) if m else piece
            number += 1
    total = answers[0]
    for m in sorted(answers)[1:]:
        total = total + answers[m].astype(TOTAL)
    return total.astype(jnp.bfloat16)


def solution(mesh):
    in_specs = (
        P(("groups", "ep"), "sub"),
        P(("groups", "ep"), None),
        P(("groups", "ep"), None),
        P("ep", "sub", None),
        P("ep", "sub", None),
        P("ep", None, "sub"),
        P("ep", "sub"),
        P("ep", "sub"),
        P("ep", "sub"),
    )
    out_specs = P(("groups", "ep"), "sub")

    return jax.shard_map(
        per_device, mesh=mesh, in_specs=in_specs, out_specs=out_specs, check_vma=False
    )
```
